32 devices in a mesh: wide: 8 (over z, core), narrow: 4 (over y, x).
Axes of the slice: x: 2, y: 2, z: 4, core: 2. Of those that a mesh axis runs over, the one named last changes fastest.
Arguments:
- operator: bfloat16 [8, 4, 2, 2048, 2048], P('wide', 'narrow'), may hold values from -0.125 to 0.125
- sources: bfloat16 [8, 4, 2048, 128], P('wide', 'narrow'), may hold values from -6 to 6
- face_lengths: int32 [8, 4, 4], P('wide', 'narrow'), may hold values from 192 to 640, as said below
Outputs:
- outgoing: bfloat16 [8, 4, 2048, 128], P('wide', 'narrow')
- incoming: bfloat16 [8, 4, 2048, 128], P('wide', 'narrow')
The draws below stay inside these ranges and needn't reach their ends.
Inputs may be any that keep to these rules, and one draw needn't show every extreme that they name: `face_lengths`: the entries of adjacent subdomains for their common face are equal; lower-row and higher-row entries lie in 320 to 640, column entries in 192 to 384.
All inputs are finite; a program needn't handle non-finite values.
Results may differ from the reference program's by a relative error of at most 0.0055.
Values may be sent and summed in bfloat16 or wider, within the bound.
A program may use at most 64 MiB of HBM per device.

```python
import jax
import jax.numpy as jnp
from jax import lax

FACE_LONG = 640
FACE_SHORT = 384
SOURCES = 64
ITERS = 3
MMAX = 2048
SUB_ROWS = 8
SUB_COLS = 4


def draw_face_lengths(key, part):
    first_key, second_key = jax.random.split(jax.random.fold_in(key, 17))
    longs = jax.random.randint(first_key, (SUB_ROWS + 1, SUB_COLS), FACE_LONG // 2, FACE_LONG + 1)
    shorts = jax.random.randint(second_key, (SUB_ROWS, SUB_COLS + 1), FACE_SHORT // 2, FACE_SHORT + 1)
    longs = longs.at[0, 0].set(FACE_LONG).at[SUB_ROWS, SUB_COLS - 1].set(FACE_LONG // 2)
    shorts = shorts.at[0, 0].set(FACE_SHORT).at[SUB_ROWS - 1, SUB_COLS].set(FACE_SHORT // 2)
    stacked = jnp.stack([longs[:-1], longs[1:], shorts[:, :-1], shorts[:, 1:]], axis=-1)
    return stacked.astype(jnp.int32)


def block_scale(key, shape, pieces, smallest, top_value):
    def one(axis_at, shards_of):
        draws = jax.random.uniform(jax.random.fold_in(jax.random.fold_in(key, 6), axis_at), (shards_of,), jnp.float32, smallest / len(pieces), top_value / len(pieces))
        return jnp.repeat(jnp.exp(draws), shape[axis_at] // shards_of).reshape((-1,) + (1,) * (len(shape) - axis_at - 1))

    loudness = one(*pieces[0])
    for cut in pieces[1:]:
        loudness = loudness * one(*cut)
    return loudness


def centred(key, shape, scale, limit, shards=(), held_as=jnp.bfloat16):
    values = scale * jax.random.normal(key, shape, jnp.float32)
    if shards:
        values = values * block_scale(key, shape, shards, -0.22, 0.18)
    return jnp.clip(values, -limit, limit).astype(held_as)


def setup_inputs(seed: int = 0) -> dict:
    splits = jax.random.split(jax.random.key(seed), 4)
    return {
        "operator": centred(splits[0], (SUB_ROWS, SUB_COLS, 2, MMAX, MMAX), MMAX ** -0.5, 0.125, ((0, 8), (1, 4))),
        "sources": centred(splits[1], (SUB_ROWS, SUB_COLS, MMAX, 2 * SOURCES), 1.0, 6.0, ((0, 8), (1, 4))),
        "face_lengths": draw_face_lengths(jax.random.fold_in(splits[3], 71), 0),
    }


def live_rows(counts):
    total = 2 * FACE_LONG + 2 * FACE_SHORT
    rows = jnp.arange(total, dtype=jnp.int32)
    edges = [0, FACE_LONG, 2 * FACE_LONG, 2 * FACE_LONG + FACE_SHORT]
    live = jnp.zeros((total,), dtype=bool)
    for face in range(4):
        live = live | ((rows >= edges[face]) & (rows < edges[face] + counts[face]))
    return live[:, None]


def trade_all(out):
    low = FACE_LONG
    mid = 2 * FACE_LONG
    high = 2 * FACE_LONG + FACE_SHORT
    lower_face = out[:, :, :low]
    upper_face = out[:, :, low:mid]
    left_face = out[:, :, mid:high]
    right_face = out[:, :, high:]
    zero_row = jnp.zeros_like(upper_face[:1])
    from_lower = jnp.concatenate([zero_row, upper_face[:-1]], axis=0)
    from_upper = jnp.concatenate([lower_face[1:], zero_row], axis=0)
    zero_col = jnp.zeros_like(right_face[:, :1])
    from_left = jnp.concatenate([zero_col, right_face[:, :-1]], axis=1)
    from_right = jnp.concatenate([left_face[:, 1:], zero_col], axis=1)
    return jnp.concatenate([from_lower, from_upper, from_left, from_right], axis=2)


def product(pair):
    oper, field = pair
    total = oper.shape[-1]
    half = field.shape[1] // 2
    stacked = oper.reshape(2 * total, total).astype(jnp.float32)
    both = jnp.dot(stacked, field.astype(jnp.float32), precision=lax.Precision.HIGHEST)
    first = both[:total]
    second = both[total:]
    real_part = first[:, :half] - second[:, half:]
    imag_part = first[:, half:] + second[:, :half]
    return jnp.concatenate([real_part, imag_part], axis=1)


def reference(operator, sources, face_lengths):
    rows_grid, cols_grid = operator.shape[0], operator.shape[1]
    total = operator.shape[-1]
    width = sources.shape[-1]
    count = rows_grid * cols_grid
    live = jax.vmap(live_rows)(face_lengths.reshape(count, 4)).reshape(rows_grid, cols_grid, total, 1)
    masked = jnp.where(live, sources, jnp.zeros_like(sources))
    incoming = trade_all(masked)
    oper_flat = operator.reshape(count, 2, total, total)
    outgoing = masked
    for step in range(ITERS):
        terms = lax.map(product, (oper_flat, incoming.reshape(count, total, width)))
        terms = terms.reshape(rows_grid, cols_grid, total, width) + sources.astype(jnp.float32)
        outgoing = jnp.where(live, terms, jnp.zeros_like(terms)).astype(jnp.bfloat16)
        incoming = trade_all(outgoing)
    return outgoing, incoming
```

```python
import functools

import jax
import jax.numpy as jnp
from jax import lax
from jax.experimental import pallas as pl
from jax.experimental.pallas import tpu as pltpu
from jax.sharding import PartitionSpec as P

FACE_LONG = 640
FACE_SHORT = 384
ITERS = 3
TILE = 512
MESH = pl.DeviceIdType.MESH


def kernel(n_wide, n_narrow, oper_hbm, src_hbm, len_ref, out_hbm, inc_hbm,
           w, src, xs, x2, acc, outs, zeros,
           w_sem, ws_sem, src_sem, send_sem, recv_sem, fin_sem, zero_sem):
    total = src.shape[0]
    short0 = 2 * FACE_LONG
    row = lax.axis_index("wide")
    col = lax.axis_index("narrow")
    far = lax.rem(row, 2)
    near = 1 - far
    first = jnp.where(2 * col < n_narrow, 1, 0)
    second = 1 - first

    def long_off(face):
        return pl.multiple_of(face * FACE_LONG, 128)

    def short_off(face):
        return pl.multiple_of(short0 + face * FACE_SHORT, 128)

    def geometry(is_long, face):
        if is_long:
            target = row + 2 * face - 1
            return (long_off(face), long_off(1 - face), FACE_LONG, {"wide": target},
                    (target >= 0) & (target < n_wide), face)
        target = col + 2 * face - 1
        return (short_off(face), short_off(1 - face), FACE_SHORT, {"narrow": target},
                (target >= 0) & (target < n_narrow), 2 + face)

    faces = [(False, first), (False, second), (True, far), (True, near)]

    def send(step, is_long, face, start):
        here, there, size, device, exists, slot = geometry(is_long, face)
        other = (2 + 1 - face) if is_long is False else 1 - face
        source = src if step == 0 else outs.at[step - 1]
        target = inc_hbm if step == ITERS else xs.at[step]
        copy = pltpu.make_async_remote_copy(
            src_ref=source.at[pl.ds(here, size)],
            dst_ref=target.at[pl.ds(there, size)],
            send_sem=send_sem.at[step, slot],
            recv_sem=recv_sem.at[step, other],
            device_id=device,
            device_id_type=MESH,
        )

        @pl.when(exists)
        def _():
            if start:
                copy.start()
            else:
                copy.wait_send()

    def receive(step, is_long, face):
        here, there, size, device, exists, slot = geometry(is_long, face)
        source = src if step == 0 else outs.at[step - 1]
        target = inc_hbm if step == ITERS else xs.at[step]
        copy = pltpu.make_async_remote_copy(
            src_ref=source.at[pl.ds(here, size)],
            dst_ref=target.at[pl.ds(here, size)],
            send_sem=send_sem.at[step, slot],
            recv_sem=recv_sem.at[step, slot],
            device_id=device,
            device_id_type=MESH,
        )

        @pl.when(exists)
        def _():
            copy.wait_recv()

    src_copy = pltpu.make_async_copy(src_hbm.at[0, 0], src, src_sem)
    src_copy.start()

    barrier = pltpu.get_barrier_semaphore()
    count = jnp.int32(0)
    for is_long, face in faces:
        _, _, _, device, exists, _ = geometry(is_long, face)
        count = count + exists.astype(jnp.int32)

        @pl.when(exists)
        def _():
            pl.semaphore_signal(barrier, inc=1, device_id=device, device_id_type=MESH)

    def load_long(which, face, tile):
        rows = pl.ds(pl.multiple_of(tile * TILE, TILE), TILE)
        cols = pl.ds(long_off(face), FACE_LONG)
        return pltpu.make_async_copy(
            oper_hbm.at[0, 0, :, rows, cols], w.at[:, rows, cols], w_sem.at[which, tile])

    def load_short():
        cols = pl.ds(short0, 2 * FACE_SHORT)
        return pltpu.make_async_copy(
            oper_hbm.at[0, 0, :, :, cols], w.at[:, :, cols], ws_sem)

    tiles = total // TILE
    for tile in range(tiles):
        load_long(0, near, tile).start()

    pl.semaphore_wait(barrier, count)
    src_copy.wait()
    for is_long, face in faces:
        send(0, is_long, face, True)

    for tile in range(tiles):
        load_long(1, far, tile).start()
    load_short().start()

    zeros[...] = jnp.zeros_like(zeros)
    for is_long, face in faces:
        here, _, size, _, exists, slot = geometry(is_long, face)

        @pl.when(jnp.logical_not(exists))
        def _():
            for step in range(ITERS):
                xs[step, pl.ds(here, size), :] = jnp.zeros((size, xs.shape[2]), xs.dtype)
            pltpu.make_async_copy(
                zeros.at[pl.ds(0, size)], inc_hbm.at[pl.ds(here, size)], zero_sem.at[slot]).start()

    def live(slot, size):
        return lax.broadcasted_iota(jnp.int32, (size, xs.shape[2]), 0) < len_ref[0, 0, slot]

    half = xs.shape[2] // 2

    def prepare(step, here, size, slot):
        value = xs[step, pl.ds(here, size), :].astype(jnp.float32)
        if step == 0:
            value = jnp.where(live(slot, size), value, 0.0)
            xs[step, pl.ds(here, size), :] = value.astype(xs.dtype)
        lanes = lax.broadcasted_iota(jnp.int32, value.shape, 1)
        turned = pltpu.roll(value, half, 1)
        x2[pl.ds(here, size), :] = jnp.where(lanes < half, -turned, turned).astype(x2.dtype)

    def product(step, rows, cols):
        return (jnp.dot(w[0, rows, cols], xs[step, cols, :], preferred_element_type=jnp.float32)
                + jnp.dot(w[1, rows, cols], x2[cols, :], preferred_element_type=jnp.float32))

    for step in range(ITERS):
        for which, face in ((0, near), (1, far)):
            receive(step, True, face)
            here = long_off(face)
            prepare(step, here, FACE_LONG, face)
            cols = pl.ds(here, FACE_LONG)

            @pl.loop(0, tiles)
            def _(tile):
                rows = pl.ds(pl.multiple_of(tile * TILE, TILE), TILE)
                if step == 0:
                    load_long(which, face, tile).wait()
                base = src[rows, :].astype(jnp.float32) if which == 0 else acc[rows, :]
                acc[rows, :] = base + product(step, rows, cols)

        if step == 0:
            load_short().wait()
        for face in (0, 1):
            receive(step, False, face)
            prepare(step, short0 + face * FACE_SHORT, FACE_SHORT, 2 + face)
        cols = pl.ds(short0, 2 * FACE_SHORT)
        for is_long, face in faces:
            here, _, size, _, _, slot = geometry(is_long, face)
            rows = pl.ds(here, size)
            value = acc[rows, :] + product(step, rows, cols)
            outs[step, rows, :] = jnp.where(live(slot, size), value, 0.0).astype(outs.dtype)
            send(step + 1, is_long, face, True)

    final = pltpu.make_async_copy(outs.at[ITERS - 1], out_hbm, fin_sem)
    final.start()
    for step in range(ITERS + 1):
        for is_long, face in faces:
            send(step, is_long, face, False)
    for is_long, face in faces:
        here, _, size, _, exists, slot = geometry(is_long, face)
        receive(ITERS, is_long, face)

        @pl.when(jnp.logical_not(exists))
        def _():
            pltpu.make_async_copy(
                zeros.at[pl.ds(0, size)], inc_hbm.at[pl.ds(here, size)], zero_sem.at[slot]).wait()
    final.wait()


def body(n_wide, n_narrow, operator, sources, face_lengths):
    total, width = sources.shape[2:]
    dtype = sources.dtype
    shape = jax.ShapeDtypeStruct((total, width), dtype)
    outgoing, incoming = pl.pallas_call(
        functools.partial(kernel, n_wide, n_narrow),
        out_shape=(shape, shape),
        in_specs=[
            pl.BlockSpec(memory_space=pl.ANY),
            pl.BlockSpec(memory_space=pl.ANY),
            pl.BlockSpec(memory_space=pltpu.SMEM),
        ],
        out_specs=[pl.BlockSpec(memory_space=pl.ANY)] * 2,
        scratch_shapes=[
            pltpu.VMEM((2, total, total), dtype),
            pltpu.VMEM((total, width), dtype),
            pltpu.VMEM((ITERS, total, width), dtype),
            pltpu.VMEM((total, width), dtype),
            pltpu.VMEM((total, width), jnp.float32),
            pltpu.VMEM((ITERS, total, width), dtype),
            pltpu.VMEM((FACE_LONG, width), dtype),
            pltpu.SemaphoreType.DMA((2, total // TILE)),
            pltpu.SemaphoreType.DMA,
            pltpu.SemaphoreType.DMA,
            pltpu.SemaphoreType.DMA((ITERS + 1, 4)),
            pltpu.SemaphoreType.DMA((ITERS + 1, 4)),
            pltpu.SemaphoreType.DMA,
            pltpu.SemaphoreType.DMA((4,)),
        ],
        compiler_params=pltpu.CompilerParams(collective_id=0, has_side_effects=True),
        name="schwarz",
    )(operator, sources, face_lengths)
    return outgoing[None, None], incoming[None, None]


def solution(mesh):
    in_specs = (
        P("wide", "narrow", None, None, None),
        P("wide", "narrow", None, None),
        P("wide", "narrow", None),
    )
    out_specs = (P("wide", "narrow", None, None), P("wide", "narrow", None, None))
    step = functools.partial(body, mesh.shape["wide"], mesh.shape["narrow"])
    return jax.shard_map(step, mesh=mesh, in_specs=in_specs, out_specs=out_specs, check_vma=False)
```

```python
import functools

import jax
import jax.numpy as jnp
from jax import lax
from jax.experimental import pallas as pl
from jax.experimental.pallas import tpu as pltpu
from jax.sharding import PartitionSpec as P

FACE_LONG = 640
FACE_SHORT = 384
ITERS = 3
TILE = 1024
MESH = pl.DeviceIdType.MESH


def kernel(n_wide, n_narrow, oper_hbm, src_hbm, len_ref, last_out, last_in,
           w, src, xs, acc, outs,
           w_sem, src_sem, send_sem, recv_sem):
    total = src.shape[0]
    short0 = 2 * FACE_LONG
    row = lax.axis_index("wide")
    col = lax.axis_index("narrow")
    far = lax.rem(row, 2)
    near = 1 - far
    first = jnp.where(2 * col < n_narrow, 1, 0)
    second = 1 - first

    def long_off(face):
        return pl.multiple_of(face * FACE_LONG, 128)

    def short_off(face):
        return pl.multiple_of(short0 + face * FACE_SHORT, 128)

    def geometry(is_long, face):
        if is_long:
            target = row + 2 * face - 1
            return (long_off(face), long_off(1 - face), FACE_LONG, {"wide": target},
                    (target >= 0) & (target < n_wide), face)
        target = col + 2 * face - 1
        return (short_off(face), short_off(1 - face), FACE_SHORT, {"narrow": target},
                (target >= 0) & (target < n_narrow), 2 + face)

    def sent_from(step):
        return src if step == 0 else last_out if step == ITERS else outs.at[step - 1]

    def landed_in(step):
        return last_in if step == ITERS else xs.at[step]

    def landing(step, there):
        return there if step == ITERS else pl.multiple_of(2 * there, 128)

    faces = [(False, first), (False, second), (True, far), (True, near)]

    def send(step, is_long, face, start):
        here, there, size, device, exists, slot = geometry(is_long, face)
        other = (2 + 1 - face) if is_long is False else 1 - face
        source, target = sent_from(step), landed_in(step)
        copy = pltpu.make_async_remote_copy(
            src_ref=source.at[pl.ds(here, size)],
            dst_ref=target.at[pl.ds(landing(step, there), size)],
            send_sem=send_sem.at[step, slot],
            recv_sem=recv_sem.at[step, other],
            device_id=device,
            device_id_type=MESH,
        )

        @pl.when(exists)
        def _():
            if start:
                copy.start()
            else:
                copy.wait_send()

    def receive(step, is_long, face):
        here, there, size, device, exists, slot = geometry(is_long, face)
        source, target = sent_from(step), landed_in(step)
        copy = pltpu.make_async_remote_copy(
            src_ref=source.at[pl.ds(here, size)],
            dst_ref=target.at[pl.ds(landing(step, here), size)],
            send_sem=send_sem.at[step, slot],
            recv_sem=recv_sem.at[step, slot],
            device_id=device,
            device_id_type=MESH,
        )

        @pl.when(exists)
        def _():
            copy.wait_recv()

    src_copy = pltpu.make_async_copy(src_hbm.at[0, 0], src, src_sem)
    src_copy.start()

    barrier = pltpu.get_barrier_semaphore()
    count = jnp.int32(0)
    for is_long, face in faces:
        _, _, _, device, exists, _ = geometry(is_long, face)
        count = count + exists.astype(jnp.int32)

        @pl.when(exists)
        def _():
            pl.semaphore_signal(barrier, inc=1, device_id=device, device_id_type=MESH)

    def loads(is_long, face):
        here, _, size, _, _, slot = geometry(is_long, face)
        return [pltpu.make_async_copy(
            oper_hbm.at[0, 0, part, :, pl.ds(here, size)],
            w.at[:, pl.ds(pl.multiple_of(2 * here + part * size, 128), size)],
            w_sem.at[part, slot]) for part in range(2)]

    def load(is_long, face):
        for copy in loads(is_long, face):
            copy.start()

    def loaded(is_long, face):
        for copy in loads(is_long, face):
            copy.wait()

    load(True, near)

    pl.semaphore_wait(barrier, count)
    src_copy.wait()
    for is_long, face in faces:
        send(0, is_long, face, True)

    load(True, far)
    load(False, 0)
    load(False, 1)

    for is_long, face in faces:
        here, _, size, _, exists, slot = geometry(is_long, face)

        @pl.when(jnp.logical_not(exists))
        def _():
            for step in range(ITERS + 1):
                rows = pl.ds(landing(step, here), size)
                landed_in(step)[rows, :] = jnp.zeros((size, xs.shape[2]), xs.dtype)

    def live(slot, size):
        return lax.broadcasted_iota(jnp.int32, (size, xs.shape[2]), 0) < len_ref[0, 0, slot]

    half = xs.shape[2] // 2

    def prepare(step, is_long, face):
        here, _, size, _, _, slot = geometry(is_long, face)
        rows = pl.ds(landing(step, here), size)
        value = xs[step, rows, :].astype(jnp.float32)
        if step == 0:
            value = jnp.where(live(slot, size), value, 0.0)
            xs[step, rows, :] = value.astype(xs.dtype)
        lanes = lax.broadcasted_iota(jnp.int32, value.shape, 1)
        turned = pltpu.roll(value, half, 1)
        rows = pl.ds(pl.multiple_of(2 * here + size, 128), size)
        xs[step, rows, :] = jnp.where(lanes < half, -turned, turned).astype(xs.dtype)

    def product(step, rows, cols):
        return jnp.dot(w[rows, cols], xs[step, cols, :], preferred_element_type=jnp.float32)

    for step in range(ITERS):
        for which, face in ((0, near), (1, far)):
            if step == 0:
                loaded(True, face)
            receive(step, True, face)
            prepare(step, True, face)
            cols = pl.ds(pl.multiple_of(2 * long_off(face), 128), 2 * FACE_LONG)

            @pl.loop(0, total // TILE)
            def _(tile):
                rows = pl.ds(pl.multiple_of(tile * TILE, TILE), TILE)
                base = src[rows, :].astype(jnp.float32) if which == 0 else acc[rows, :]
                acc[rows, :] = base + product(step, rows, cols)

        for face in (0, 1):
            if step == 0:
                loaded(False, face)
        for face in (0, 1):
            receive(step, False, face)
            prepare(step, False, face)
        cols = pl.ds(2 * short0, 4 * FACE_SHORT)
        for is_long, face in faces:
            here, _, size, _, _, slot = geometry(is_long, face)
            rows = pl.ds(here, size)
            value = acc[rows, :] + product(step, rows, cols)
            sent_from(step + 1)[rows, :] = jnp.where(live(slot, size), value, 0.0).astype(xs.dtype)
            send(step + 1, is_long, face, True)

    for step in range(ITERS + 1):
        for is_long, face in faces:
            send(step, is_long, face, False)
    for is_long, face in faces:
        receive(ITERS, is_long, face)


def write_out(out_ref, in_ref, out_hbm, in_hbm, sem):
    copies = [pltpu.make_async_copy(out_ref, out_hbm.at[0, 0], sem.at[0]),
              pltpu.make_async_copy(in_ref, in_hbm.at[0, 0], sem.at[1])]
    for copy in copies:
        copy.start()
    for copy in copies:
        copy.wait()


def body(n_wide, n_narrow, operator, sources, face_lengths):
    total, width = sources.shape[2:]
    dtype = sources.dtype
    held = pltpu.VMEM((total, width), dtype)
    outgoing, incoming = pl.pallas_call(
        functools.partial(kernel, n_wide, n_narrow),
        out_shape=(held, held),
        in_specs=[
            pl.BlockSpec(memory_space=pltpu.HBM),
            pl.BlockSpec(memory_space=pltpu.HBM),
            pl.BlockSpec(memory_space=pltpu.SMEM),
        ],
        out_specs=[pl.BlockSpec(memory_space=pltpu.VMEM)] * 2,
        scratch_shapes=[
            pltpu.VMEM((total, 2 * total), dtype),
            pltpu.VMEM((total, width), dtype),
            pltpu.VMEM((ITERS, 2 * total, width), dtype),
            pltpu.VMEM((total, width), jnp.float32),
            pltpu.VMEM((ITERS - 1, total, width), dtype),
            pltpu.SemaphoreType.DMA((2, 4)),
            pltpu.SemaphoreType.DMA,
            pltpu.SemaphoreType.DMA((ITERS + 1, 4)),
            pltpu.SemaphoreType.DMA((ITERS + 1, 4)),
        ],
        compiler_params=pltpu.CompilerParams(
            collective_id=0, has_side_effects=True, vmem_limit_bytes=54 * 1024 * 1024),
        name="schwarz",
    )(operator, sources, face_lengths)
    shape = jax.ShapeDtypeStruct(sources.shape, dtype)
    return pl.pallas_call(
        write_out,
        out_shape=(shape, shape),
        in_specs=[pl.BlockSpec(memory_space=pltpu.VMEM)] * 2,
        out_specs=[pl.BlockSpec(memory_space=pl.ANY)] * 2,
        scratch_shapes=[pltpu.SemaphoreType.DMA((2,))],
        compiler_params=pltpu.CompilerParams(vmem_limit_bytes=4 * 1024 * 1024),
        name="write_out",
    )(outgoing, incoming)


def solution(mesh):
    in_specs = (
        P("wide", "narrow", None, None, None),
        P("wide", "narrow", None, None),
        P("wide", "narrow", None),
    )
    out_specs = (P("wide", "narrow", None, None), P("wide", "narrow", None, None))
    step = functools.partial(body, mesh.shape["wide"], mesh.shape["narrow"])
    return jax.shard_map(step, mesh=mesh, in_specs=in_specs, out_specs=out_specs, check_vma=False)
```
